32 devices in a mesh: pop: 2 (over x), chain: 16 (over z, y, core).
Axes of the slice: x: 2, y: 2, z: 4, core: 2. Of those that a mesh axis runs over, the one named last changes fastest.
Arguments:
- cost: float32 [8192, 4096], P(('pop', 'chain')), parts along dimension 0, may hold values from 0 to 20
- marginals: float32 [8192], P(('pop', 'chain')), parts along dimension 0, may hold values from 0.125 to 6
- final_marginal: float32 [8192], P('pop'), parts along dimension 0, may hold values from 0.125 to 6
Outputs:
- log_scaling: float32 [8192], P(('pop', 'chain')), parts along dimension 0
The draws below stay inside these ranges and needn't reach their ends.
There are 2 independent parts, one for each index of `pop`. The reference program is written for one: setup_inputs(seed, part) draws one part's arguments, and reference() takes and returns one part's arrays. A program takes and returns all parts, laid end to end along the dimension named above; each array names one. Nothing has to cross between parts.
All inputs are finite; a program needn't handle non-finite values.
Results may differ from the reference program's by a relative error of at most 0.0001.
Values sent between devices are 32-bit elements; how exact they have to be, the bound alone decides.
No kernel may reach another device: no remote copies, remote signals or barrier semaphores. Data moves between devices by JAX's collectives and lax.ppermute only.
A program may use at most 64 MiB of HBM per device.

```python
import math
import jax
import jax.numpy as jnp
from jax import lax

STATES = 4096
SWEEPS = 2
KERNELS = 1


def ramped_mass(key, entries):
    base_key = jax.random.fold_in(key, 11)
    baseline = jnp.exp(jax.random.uniform(base_key, (entries,), jnp.float32, math.log(0.25), math.log(4.0)))
    position = (jnp.arange(entries) % STATES).astype(jnp.float32)
    return baseline * (0.5 + position / STATES)


def draw_marginals(key, part):
    return ramped_mass(jax.random.fold_in(key, 3), KERNELS * STATES)


def draw_final_marginal(key, part):
    return ramped_mass(jax.random.fold_in(key, 5), STATES)


def draw_cost(key, part):
    row_total = KERNELS * STATES
    rough_key = jax.random.fold_in(key, 21)
    offset_key = jax.random.fold_in(key, 22)
    block_key = jax.random.fold_in(key, 23)
    rough_draw = jax.random.uniform(rough_key, (row_total, STATES), jnp.float32, 0.0, 1.0)
    offset_draw = jax.random.uniform(offset_key, (row_total, 1), jnp.float32, 0.0, 1.0)
    roughness = 12.0 * rough_draw
    row_offset = 4.0 * offset_draw
    block_draw = jax.random.uniform(block_key, (KERNELS, 4, 4), jnp.float32, 0.0, 1.0)
    diagonal_mask = jnp.eye(4, dtype=jnp.float32)
    block_cost = diagonal_mask * (0.5 * block_draw) + (1.0 - diagonal_mask) * (2.5 + block_draw)
    row_index = jnp.arange(row_total)
    kernel_index = row_index // STATES
    row_cluster = row_index % STATES * 4 // STATES
    column_cluster = jnp.arange(STATES) * 4 // STATES
    block_rows = block_cost[kernel_index, row_cluster]
    penalty = jnp.take(block_rows, column_cluster, axis=1)
    return jnp.clip(roughness + row_offset + penalty, 0.0, 20.0)


def setup_inputs(seed: int = 0, part: int = 0) -> dict:
    arg_keys = jax.random.split(jax.random.key(seed), 4)
    part_splits = jax.random.split(jax.random.fold_in(arg_keys[3], part), 4)
    cost = draw_cost(jax.random.fold_in(jax.random.fold_in(arg_keys[3], part), 71), part)
    marginals = draw_marginals(jax.random.fold_in(jax.random.fold_in(arg_keys[3], part), 71), part)
    final_marginal = draw_final_marginal(jax.random.fold_in(jax.random.fold_in(arg_keys[3], part), 71), part)
    return {"cost": cost, "marginals": marginals, "final_marginal": final_marginal}


entropic = 0.25


def reference(cost, marginals, final_marginal):
    kernel = jnp.exp(-cost / entropic).reshape(KERNELS, STATES, STATES)
    target = marginals.reshape(KERNELS, STATES)
    scaling = jnp.ones((KERNELS, STATES), jnp.float32)
    last_scaling = jnp.ones((STATES,), jnp.float32)
    for sweep_index in range(SWEEPS):
        alphas = [jnp.ones((STATES,), jnp.float32)]
        for position in range(KERNELS):
            message = jnp.dot(scaling[position] * alphas[position], kernel[position],
                              precision=lax.Precision.HIGHEST, preferred_element_type=jnp.float32)
            alphas.append(message * (STATES / jnp.sum(message)))
        betas = [jnp.ones((STATES,), jnp.float32) for position in range(KERNELS)]
        carried = last_scaling
        for position in reversed(range(KERNELS)):
            message = jnp.dot(kernel[position], carried,
                              precision=lax.Precision.HIGHEST, preferred_element_type=jnp.float32)
            betas[position] = message * (STATES / jnp.sum(message))
            carried = scaling[position] * betas[position]
        scaling = target / (jnp.stack(alphas[:KERNELS]) * jnp.stack(betas))
        last_scaling = final_marginal / alphas[KERNELS]
    return jnp.log(scaling).reshape(KERNELS * STATES)
```

```python
import jax
import jax.numpy as jnp
from jax import lax
from jax.experimental import pallas as pl
from jax.experimental.pallas import tpu as pltpu
from jax.sharding import PartitionSpec as P

SWEEPS = 2
LANES = 128
SUBLANES = 8
CHUNKS = 8


entropic = 0.25
EXP2_SCALE = -1.4426950408889634 / entropic


def swapped(value, axis, apart):
    return lax.ppermute(value, axis, [(i, i ^ apart) for i in range(lax.axis_size(axis))])


def distances(width):
    return [1 << bit_index | 1 for bit_index in range(width.bit_length() - 1)]


def butterfly_sum(vector, width):
    for apart in distances(width):
        vector = vector + swapped(vector, "chain", apart)
    return vector


def kernel_and_sums(cost):
    rows, states = cost.shape
    tiles = states // LANES
    chunk = rows // CHUNKS

    def body(cost_ref, kernel_ref, sums_ref, sems):
        def copy(index):
            span = pl.ds(index * chunk, chunk)
            return pltpu.make_async_copy(cost_ref.at[span], kernel_ref.at[span], sems.at[index])

        for index in range(CHUNKS):
            copy(index).start()
        totals = [jnp.zeros((SUBLANES, LANES), jnp.float32)] * tiles
        for index in range(CHUNKS):
            copy(index).wait()
            for first in range(index * chunk, (index + 1) * chunk, SUBLANES):
                for tile in range(tiles):
                    at = (pl.ds(first, SUBLANES), pl.ds(tile * LANES, LANES))
                    value = jnp.exp2(kernel_ref[at] * EXP2_SCALE)
                    kernel_ref[at] = value
                    totals[tile] = totals[tile] + value
        for tile in range(tiles):
            sums_ref[pl.ds(tile, 1), :] = jnp.sum(totals[tile], axis=0, keepdims=True)

    return pl.pallas_call(
        body,
        out_shape=(
            jax.ShapeDtypeStruct((rows, states), jnp.float32),
            jax.ShapeDtypeStruct((tiles, LANES), jnp.float32),
        ),
        in_specs=[pl.BlockSpec(memory_space=pltpu.HBM)],
        out_specs=[pl.BlockSpec(memory_space=pltpu.VMEM)] * 2,
        scratch_shapes=[pltpu.SemaphoreType.DMA((CHUNKS,))],
        compiler_params=pltpu.CompilerParams(vmem_limit_bytes=16 << 20),
        name="kernel_and_sums",
    )(cost)


def log_row_scaling(kernel, half, other_half, final_marginal, marginals):
    rows, states = kernel.shape
    tiles = states // LANES

    def body(kernel_ref, half_ref, other_ref, final_ref, marginal_ref, out_ref, weight_ref):
        final = final_ref[...]
        weight_ref[...] = final * float(states) / (half_ref[...] + other_ref[...])
        total = jnp.sum(final, keepdims=True)
        weights = [
            jnp.broadcast_to(weight_ref[pl.ds(tile, 1), :], (SUBLANES, LANES)) for tile in range(tiles)
        ]
        partial = []
        for first in range(0, rows, SUBLANES):
            sums = [None] * 4
            for tile in range(tiles):
                at = (pl.ds(first, SUBLANES), pl.ds(tile * LANES, LANES))
                term = kernel_ref[at] * weights[tile]
                sums[tile % 4] = term if sums[tile % 4] is None else sums[tile % 4] + term
            partial.append((sums[0] + sums[1]) + (sums[2] + sums[3]))
        for block in range(rows // LANES):
            square = jnp.concatenate(partial[block * 16 : block * 16 + 16], axis=0)
            row_sums = jnp.sum(square.T, axis=0, keepdims=True)
            at = (pl.ds(block, 1), slice(None))
            out_ref[at] = jnp.log(marginal_ref[at] * total / row_sums)

    return pl.pallas_call(
        body,
        out_shape=jax.ShapeDtypeStruct((rows // LANES, LANES), jnp.float32),
        in_specs=[pl.BlockSpec(memory_space=pltpu.VMEM)] * 5,
        out_specs=pl.BlockSpec(memory_space=pltpu.VMEM),
        scratch_shapes=[pltpu.VMEM((tiles, LANES), jnp.float32)],
        compiler_params=pltpu.CompilerParams(vmem_limit_bytes=16 << 20),
        name="log_row_scaling",
    )(
        kernel,
        half,
        other_half,
        final_marginal.reshape(tiles, LANES),
        marginals.reshape(rows // LANES, LANES),
    ).reshape(rows)


def one_kernel(cost, marginals, final_marginal):
    width = cost.shape[1] // cost.shape[0]
    kernel, sums = kernel_and_sums(cost)
    *early, last = distances(width)
    for apart in early:
        sums = sums + swapped(sums, "chain", apart)
    return log_row_scaling(kernel, sums, swapped(sums, "chain", last), final_marginal, marginals)


def from_behind(block, axis, distance):
    devices = range(lax.axis_size(axis))
    route = [(i - distance, i) for i in devices if i - distance in devices]
    return lax.ppermute(block, axis, route)


def doubling_gather(first, second, member, width):
    for bit_index in range(width.bit_length() - 1):
        other_first, other_second = (swapped(part, "chain", 1 << bit_index) for part in (first, second))
        upward = member >> bit_index & 1 == 1
        first = jnp.where(
            upward, jnp.concatenate([other_first, first]), jnp.concatenate([first, other_first])
        )
        second = jnp.where(
            upward, jnp.concatenate([other_second, second]), jnp.concatenate([second, other_second])
        )
    return (first, second)


def many_kernels(cost, marginals, final_marginal):
    row_count = cost.shape[0]
    states = cost.shape[1]
    width = states // row_count
    kernels = lax.axis_size("chain") // width
    index = lax.axis_index("chain")
    group = index // width
    member = index % width
    kernel = jnp.exp(-cost / entropic)
    scaling = jnp.ones((row_count,), jnp.float32)
    last_scaling = jnp.ones((states,), jnp.float32)
    for sweep_index in range(SWEEPS):
        current = scaling
        alpha_start = jnp.ones((states,), jnp.float32)
        forward_state = (jnp.ones((row_count,), jnp.float32), current, alpha_start)
        backward_state = (jnp.ones((row_count,), jnp.float32), last_scaling)
        for position in range(kernels):
            partial_sums = jnp.dot(
                forward_state[1],
                kernel,
                precision=lax.Precision.HIGHEST,
                preferred_element_type=jnp.float32,
            )
            whole = butterfly_sum(partial_sums, width)
            forward_whole_alpha = whole * (states / jnp.sum(whole))
            forward_outgoing = lax.dynamic_slice_in_dim(
                forward_whole_alpha, member * row_count, row_count
            )
            forward_alpha_block, carried, forward_alpha_last = forward_state
            if position == kernels - 1:
                forward_alpha_last = forward_whole_alpha
            if position < kernels - 1:
                forward_arrived = from_behind(forward_outgoing, "chain", width)
                taking = group == position + 1
                forward_alpha_block = jnp.where(taking, forward_arrived, forward_alpha_block)
                carried = jnp.where(taking, current * forward_arrived, carried)
            forward_state = (forward_alpha_block, carried, forward_alpha_last)
        for position in range(kernels):
            backward_raw = jnp.dot(
                kernel,
                backward_state[1],
                precision=lax.Precision.HIGHEST,
                preferred_element_type=jnp.float32,
            )
            backward_raw_full, backward_weighted_full = doubling_gather(
                backward_raw, current * backward_raw, member, width
            )
            backward_beta_block, carried_full = backward_state
            target_step = kernels - 1 - position
            factor = states / jnp.sum(backward_raw_full)
            backward_beta_block = jnp.where(
                group == target_step, backward_raw * factor, backward_beta_block
            )
            if target_step > 0:
                arrived = from_behind(backward_weighted_full * factor, "chain", -width)
                carried_full = jnp.where(group == target_step - 1, arrived, carried_full)
            backward_state = (backward_beta_block, carried_full)
        alpha_block, carried_unused, alpha_last = forward_state
        beta_block = backward_state[0]
        scaling = marginals / (alpha_block * beta_block)
        last_scaling = final_marginal / alpha_last
    return jnp.log(scaling)


def on_device(cost, marginals, final_marginal):
    width = cost.shape[1] // cost.shape[0]
    if lax.axis_size("chain") == width:
        return one_kernel(cost, marginals, final_marginal)
    return many_kernels(cost, marginals, final_marginal)


def solution(mesh):
    placed = (P(("pop", "chain"), None), P(("pop", "chain")), P("pop"))
    return jax.shard_map(
        on_device, mesh=mesh, in_specs=placed, out_specs=P(("pop", "chain")), check_vma=False
    )
```

```python
import jax
import jax.numpy as jnp
from jax import lax
from jax.experimental import pallas as pl
from jax.experimental.pallas import tpu as pltpu
from jax.sharding import PartitionSpec as P

SWEEPS = 2
LANES = 128
SUBLANES = 8
CHUNKS = 8


entropic = 0.25
EXP2_SCALE = -1.4426950408889634 / entropic


def swapped(value, axis, apart):
    return lax.ppermute(value, axis, [(i, i ^ apart) for i in range(lax.axis_size(axis))])


def distances(width):
    return [1 << bit_index | 1 for bit_index in range(width.bit_length() - 1)]


def butterfly_sum(vector, width):
    for apart in distances(width):
        vector = vector + swapped(vector, "chain", apart)
    return vector


def kernel_and_sums(cost):
    rows, states = cost.shape
    tiles = states // LANES
    chunk = rows // CHUNKS

    def body(cost_ref, kernel_ref, sums_ref, sems):
        def copy(index):
            span = pl.ds(index * chunk, chunk)
            return pltpu.make_async_copy(cost_ref.at[span], kernel_ref.at[span], sems.at[index])

        for index in range(CHUNKS):
            copy(index).start()
        totals = [jnp.zeros((SUBLANES, LANES), jnp.float32)] * tiles
        for index in range(CHUNKS):
            copy(index).wait()
            for first in range(index * chunk, (index + 1) * chunk, SUBLANES):
                for tile in range(tiles):
                    at = (pl.ds(first, SUBLANES), pl.ds(tile * LANES, LANES))
                    value = jnp.exp2(kernel_ref[at] * EXP2_SCALE)
                    kernel_ref[at] = value
                    totals[tile] = totals[tile] + value
        for tile in range(tiles):
            sums_ref[pl.ds(tile, 1), :] = jnp.sum(totals[tile], axis=0, keepdims=True)

    return pl.pallas_call(
        body,
        out_shape=(
            jax.ShapeDtypeStruct((rows, states), jnp.float32),
            jax.ShapeDtypeStruct((tiles, LANES), jnp.float32),
        ),
        in_specs=[pl.BlockSpec(memory_space=pltpu.HBM)],
        out_specs=[pl.BlockSpec(memory_space=pltpu.VMEM)] * 2,
        scratch_shapes=[pltpu.SemaphoreType.DMA((CHUNKS,))],
        compiler_params=pltpu.CompilerParams(vmem_limit_bytes=16 << 20),
        name="kernel_and_sums",
    )(pltpu.with_memory_space_constraint(cost, pltpu.HBM))


def log_row_scaling(kernel, half, other_half, final_marginal, marginals):
    rows, states = kernel.shape
    tiles = states // LANES

    def body(kernel_ref, half_ref, other_ref, final_ref, marginal_ref, out_ref, weight_ref):
        final = final_ref[...]
        weight_ref[...] = final * float(states) / (half_ref[...] + other_ref[...])
        total = jnp.sum(final, keepdims=True)
        weights = [
            jnp.broadcast_to(weight_ref[pl.ds(tile, 1), :], (SUBLANES, LANES)) for tile in range(tiles)
        ]
        partial = []
        for first in range(0, rows, SUBLANES):
            sums = [None] * 4
            for tile in range(tiles):
                at = (pl.ds(first, SUBLANES), pl.ds(tile * LANES, LANES))
                term = kernel_ref[at] * weights[tile]
                sums[tile % 4] = term if sums[tile % 4] is None else sums[tile % 4] + term
            partial.append((sums[0] + sums[1]) + (sums[2] + sums[3]))
        for block in range(rows // LANES):
            square = jnp.concatenate(partial[block * 16 : block * 16 + 16], axis=0)
            row_sums = jnp.sum(square.T, axis=0, keepdims=True)
            at = (pl.ds(block, 1), slice(None))
            out_ref[at] = jnp.log(marginal_ref[at] * total / row_sums)

    return pl.pallas_call(
        body,
        out_shape=jax.ShapeDtypeStruct((rows // LANES, LANES), jnp.float32),
        in_specs=[pl.BlockSpec(memory_space=pltpu.VMEM)] * 5,
        out_specs=pl.BlockSpec(memory_space=pltpu.VMEM),
        scratch_shapes=[pltpu.VMEM((tiles, LANES), jnp.float32)],
        compiler_params=pltpu.CompilerParams(vmem_limit_bytes=16 << 20),
        name="log_row_scaling",
    )(
        kernel,
        half,
        other_half,
        final_marginal.reshape(tiles, LANES),
        marginals.reshape(rows // LANES, LANES),
    ).reshape(rows)


def one_kernel(cost, marginals, final_marginal):
    width = cost.shape[1] // cost.shape[0]
    kernel, sums = kernel_and_sums(cost)
    *early, last = distances(width)
    for apart in early:
        sums = sums + swapped(sums, "chain", apart)
    return log_row_scaling(kernel, sums, swapped(sums, "chain", last), final_marginal, marginals)


def from_behind(block, axis, distance):
    devices = range(lax.axis_size(axis))
    route = [(i - distance, i) for i in devices if i - distance in devices]
    return lax.ppermute(block, axis, route)


def doubling_gather(first, second, member, width):
    for bit_index in range(width.bit_length() - 1):
        other_first, other_second = (swapped(part, "chain", 1 << bit_index) for part in (first, second))
        upward = member >> bit_index & 1 == 1
        first = jnp.where(
            upward, jnp.concatenate([other_first, first]), jnp.concatenate([first, other_first])
        )
        second = jnp.where(
            upward, jnp.concatenate([other_second, second]), jnp.concatenate([second, other_second])
        )
    return (first, second)


def many_kernels(cost, marginals, final_marginal):
    row_count = cost.shape[0]
    states = cost.shape[1]
    width = states // row_count
    kernels = lax.axis_size("chain") // width
    index = lax.axis_index("chain")
    group = index // width
    member = index % width
    kernel = jnp.exp(-cost / entropic)
    scaling = jnp.ones((row_count,), jnp.float32)
    last_scaling = jnp.ones((states,), jnp.float32)
    for sweep_index in range(SWEEPS):
        current = scaling
        alpha_start = jnp.ones((states,), jnp.float32)
        forward_state = (jnp.ones((row_count,), jnp.float32), current, alpha_start)
        backward_state = (jnp.ones((row_count,), jnp.float32), last_scaling)
        for position in range(kernels):
            partial_sums = jnp.dot(
                forward_state[1],
                kernel,
                precision=lax.Precision.HIGHEST,
                preferred_element_type=jnp.float32,
            )
            whole = butterfly_sum(partial_sums, width)
            forward_whole_alpha = whole * (states / jnp.sum(whole))
            forward_outgoing = lax.dynamic_slice_in_dim(
                forward_whole_alpha, member * row_count, row_count
            )
            forward_alpha_block, carried, forward_alpha_last = forward_state
            if position == kernels - 1:
                forward_alpha_last = forward_whole_alpha
            if position < kernels - 1:
                forward_arrived = from_behind(forward_outgoing, "chain", width)
                taking = group == position + 1
                forward_alpha_block = jnp.where(taking, forward_arrived, forward_alpha_block)
                carried = jnp.where(taking, current * forward_arrived, carried)
            forward_state = (forward_alpha_block, carried, forward_alpha_last)
        for position in range(kernels):
            backward_raw = jnp.dot(
                kernel,
                backward_state[1],
                precision=lax.Precision.HIGHEST,
                preferred_element_type=jnp.float32,
            )
            backward_raw_full, backward_weighted_full = doubling_gather(
                backward_raw, current * backward_raw, member, width
            )
            backward_beta_block, carried_full = backward_state
            target_step = kernels - 1 - position
            factor = states / jnp.sum(backward_raw_full)
            backward_beta_block = jnp.where(
                group == target_step, backward_raw * factor, backward_beta_block
            )
            if target_step > 0:
                arrived = from_behind(backward_weighted_full * factor, "chain", -width)
                carried_full = jnp.where(group == target_step - 1, arrived, carried_full)
            backward_state = (backward_beta_block, carried_full)
        alpha_block, carried_unused, alpha_last = forward_state
        beta_block = backward_state[0]
        scaling = marginals / (alpha_block * beta_block)
        last_scaling = final_marginal / alpha_last
    return jnp.log(scaling)


def on_device(cost, marginals, final_marginal):
    width = cost.shape[1] // cost.shape[0]
    if lax.axis_size("chain") == width:
        return one_kernel(cost, marginals, final_marginal)
    return many_kernels(cost, marginals, final_marginal)


def solution(mesh):
    placed = (P(("pop", "chain"), None), P(("pop", "chain")), P("pop"))
    return jax.shard_map(
        on_device, mesh=mesh, in_specs=placed, out_specs=P(("pop", "chain")), check_vma=False
    )
```

```python
import jax
import jax.numpy as jnp
from jax import lax
from jax.experimental import pallas as pl
from jax.experimental.pallas import tpu as pltpu
from jax.sharding import PartitionSpec as P

SWEEPS = 2
LANES = 128
SUBLANES = 8
CHUNKS = 8


entropic = 0.25
EXP2_SCALE = -1.4426950408889634 / entropic


def swapped(value, axis, apart):
    return lax.ppermute(value, axis, [(i, i ^ apart) for i in range(lax.axis_size(axis))])


def stages(width):
    across = [1 << bit_index | 1 for bit_index in range(1, width.bit_length() - 1)]
    if len(across) < 2:
        return [[(apart, apart)] for apart in [*across, 1] if apart < width]
    one, other, *rest = across
    both = one ^ other | 1
    last = [(both, both), (one, other), (other, one)]
    return [*([(apart, apart)] for apart in rest), [(1, 1)], last]


def exchanged(value, stage):
    devices = range(lax.axis_size("chain"))
    return [
        lax.ppermute(value, "chain", [(i, i ^ (odd if i & 1 else even)) for i in devices])
        for odd, even in stage
    ]


def butterfly_sum(vector, width):
    for stage in stages(width):
        vector = sum(exchanged(vector, stage), vector)
    return vector


def kernel_and_sums(cost, final_marginal, marginals):
    rows, states = cost.shape
    tiles = states // LANES
    chunk = rows // CHUNKS

    def body(cost_ref, final_ref, marginal_ref, kernel_ref, sums_ref, scaled_ref, target_ref, sems, small_sems):
        def copy(index):
            span = pl.ds(index * chunk, chunk)
            return pltpu.make_async_copy(cost_ref.at[span], kernel_ref.at[span], sems.at[index])

        small = (
            pltpu.make_async_copy(final_ref, scaled_ref, small_sems.at[0]),
            pltpu.make_async_copy(marginal_ref, target_ref, small_sems.at[1]),
        )
        for index in range(CHUNKS):
            copy(index).start()
        for each in small:
            each.start()
        totals = [jnp.zeros((SUBLANES, LANES), jnp.float32)] * tiles
        for index in range(CHUNKS):
            copy(index).wait()
            if index == CHUNKS - 2:
                for each in small:
                    each.wait()
                final = scaled_ref[...]
                scaled_ref[...] = final * float(states)
                target_ref[...] = target_ref[...] * jnp.sum(final, keepdims=True)
            for first in range(index * chunk, (index + 1) * chunk, SUBLANES):
                for tile in range(tiles):
                    at = (pl.ds(first, SUBLANES), pl.ds(tile * LANES, LANES))
                    value = jnp.exp2(kernel_ref[at] * EXP2_SCALE)
                    kernel_ref[at] = value
                    totals[tile] = totals[tile] + value
        for tile in range(tiles):
            sums_ref[pl.ds(tile, 1), :] = jnp.sum(totals[tile], axis=0, keepdims=True)

    operands = (cost, final_marginal.reshape(tiles, LANES), marginals.reshape(rows // LANES, LANES))
    shapes = ((rows, states), (tiles, LANES), (tiles, LANES), (rows // LANES, LANES))
    return pl.pallas_call(
        body,
        out_shape=[jax.ShapeDtypeStruct(shape, jnp.float32) for shape in shapes],
        in_specs=[pl.BlockSpec(memory_space=pltpu.HBM)] * 3,
        out_specs=[pl.BlockSpec(memory_space=pltpu.VMEM)] * 4,
        scratch_shapes=[pltpu.SemaphoreType.DMA((CHUNKS,)), pltpu.SemaphoreType.DMA((2,))],
        compiler_params=pltpu.CompilerParams(vmem_limit_bytes=16 << 20),
        name="kernel_and_sums",
    )(*(pltpu.with_memory_space_constraint(operand, pltpu.HBM) for operand in operands))


def log_row_scaling(kernel, parts, scaled, target):
    rows, states = kernel.shape
    tiles = states // LANES

    def body(kernel_ref, scaled_ref, target_ref, *refs):
        *part_refs, out_ref, weight_ref = refs
        sums = sum((ref[...] for ref in part_refs[1:]), part_refs[0][...])
        weight_ref[...] = scaled_ref[...] / sums
        weights = [
            jnp.broadcast_to(weight_ref[pl.ds(tile, 1), :], (SUBLANES, LANES)) for tile in range(tiles)
        ]
        partial = []
        for first in range(0, rows, SUBLANES):
            sums = [None] * 4
            for tile in range(tiles):
                at = (pl.ds(first, SUBLANES), pl.ds(tile * LANES, LANES))
                term = kernel_ref[at] * weights[tile]
                sums[tile % 4] = term if sums[tile % 4] is None else sums[tile % 4] + term
            partial.append((sums[0] + sums[1]) + (sums[2] + sums[3]))
        for block in range(rows // LANES):
            square = jnp.concatenate(partial[block * 16 : block * 16 + 16], axis=0)
            row_sums = jnp.sum(square.T, axis=0, keepdims=True)
            at = (pl.ds(block, 1), slice(None))
            out_ref[at] = jnp.log(target_ref[at] / row_sums)

    return pl.pallas_call(
        body,
        out_shape=jax.ShapeDtypeStruct((rows // LANES, LANES), jnp.float32),
        in_specs=[pl.BlockSpec(memory_space=pltpu.VMEM)] * (3 + len(parts)),
        out_specs=pl.BlockSpec(memory_space=pltpu.VMEM),
        scratch_shapes=[pltpu.VMEM((tiles, LANES), jnp.float32)],
        compiler_params=pltpu.CompilerParams(vmem_limit_bytes=16 << 20),
        name="log_row_scaling",
    )(kernel, scaled, target, *parts).reshape(rows)


def one_kernel(cost, marginals, final_marginal):
    width = cost.shape[1] // cost.shape[0]
    kernel, sums, scaled, target = kernel_and_sums(cost, final_marginal, marginals)
    *early, last = stages(width)
    for stage in early:
        sums = sum(exchanged(sums, stage), sums)
    return log_row_scaling(kernel, [sums, *exchanged(sums, last)], scaled, target)


def from_behind(block, axis, distance):
    devices = range(lax.axis_size(axis))
    route = [(i - distance, i) for i in devices if i - distance in devices]
    return lax.ppermute(block, axis, route)


def doubling_gather(first, second, member, width):
    for bit_index in range(width.bit_length() - 1):
        other_first, other_second = (swapped(part, "chain", 1 << bit_index) for part in (first, second))
        upward = member >> bit_index & 1 == 1
        first = jnp.where(
            upward, jnp.concatenate([other_first, first]), jnp.concatenate([first, other_first])
        )
        second = jnp.where(
            upward, jnp.concatenate([other_second, second]), jnp.concatenate([second, other_second])
        )
    return (first, second)


def many_kernels(cost, marginals, final_marginal):
    row_count = cost.shape[0]
    states = cost.shape[1]
    width = states // row_count
    kernels = lax.axis_size("chain") // width
    index = lax.axis_index("chain")
    group = index // width
    member = index % width
    kernel = jnp.exp(-cost / entropic)
    scaling = jnp.ones((row_count,), jnp.float32)
    last_scaling = jnp.ones((states,), jnp.float32)
    for sweep_index in range(SWEEPS):
        current = scaling
        alpha_start = jnp.ones((states,), jnp.float32)
        forward_state = (jnp.ones((row_count,), jnp.float32), current, alpha_start)
        backward_state = (jnp.ones((row_count,), jnp.float32), last_scaling)
        for position in range(kernels):
            partial_sums = jnp.dot(
                forward_state[1],
                kernel,
                precision=lax.Precision.HIGHEST,
                preferred_element_type=jnp.float32,
            )
            whole = butterfly_sum(partial_sums, width)
            forward_whole_alpha = whole * (states / jnp.sum(whole))
            forward_outgoing = lax.dynamic_slice_in_dim(
                forward_whole_alpha, member * row_count, row_count
            )
            forward_alpha_block, carried, forward_alpha_last = forward_state
            if position == kernels - 1:
                forward_alpha_last = forward_whole_alpha
            if position < kernels - 1:
                forward_arrived = from_behind(forward_outgoing, "chain", width)
                taking = group == position + 1
                forward_alpha_block = jnp.where(taking, forward_arrived, forward_alpha_block)
                carried = jnp.where(taking, current * forward_arrived, carried)
            forward_state = (forward_alpha_block, carried, forward_alpha_last)
        for position in range(kernels):
            backward_raw = jnp.dot(
                kernel,
                backward_state[1],
                precision=lax.Precision.HIGHEST,
                preferred_element_type=jnp.float32,
            )
            backward_raw_full, backward_weighted_full = doubling_gather(
                backward_raw, current * backward_raw, member, width
            )
            backward_beta_block, carried_full = backward_state
            target_step = kernels - 1 - position
            factor = states / jnp.sum(backward_raw_full)
            backward_beta_block = jnp.where(
                group == target_step, backward_raw * factor, backward_beta_block
            )
            if target_step > 0:
                arrived = from_behind(backward_weighted_full * factor, "chain", -width)
                carried_full = jnp.where(group == target_step - 1, arrived, carried_full)
            backward_state = (backward_beta_block, carried_full)
        alpha_block, carried_unused, alpha_last = forward_state
        beta_block = backward_state[0]
        scaling = marginals / (alpha_block * beta_block)
        last_scaling = final_marginal / alpha_last
    return jnp.log(scaling)


def on_device(cost, marginals, final_marginal):
    width = cost.shape[1] // cost.shape[0]
    if lax.axis_size("chain") == width:
        return one_kernel(cost, marginals, final_marginal)
    return many_kernels(cost, marginals, final_marginal)


def solution(mesh):
    placed = (P(("pop", "chain"), None), P(("pop", "chain")), P("pop"))
    return jax.shard_map(
        on_device, mesh=mesh, in_specs=placed, out_specs=P(("pop", "chain")), check_vma=False
    )
```

```python
import jax
import jax.numpy as jnp
from jax import lax
from jax.experimental import pallas as pl
from jax.experimental.pallas import tpu as pltpu
from jax.sharding import PartitionSpec as P

SWEEPS = 2
LANES = 128
SUBLANES = 8
CHUNKS = 8


entropic = 0.25
EXP2_SCALE = -1.4426950408889634 / entropic


def swapped(value, axis, apart):
    return lax.ppermute(value, axis, [(i, i ^ apart) for i in range(lax.axis_size(axis))])


def distances(width):
    return [1 << bit_index | 1 for bit_index in range(1, width.bit_length() - 1)]


def stages(width):
    across = distances(width)
    if len(across) < 2:
        return [[(apart, apart)] for apart in [*across, 1] if apart < width]
    one, other, *rest = across
    both = one ^ other | 1
    last = [(both, both), (one, other), (other, one)]
    return [*([(apart, apart)] for apart in rest), [(1, 1)], last]


def exchanged(value, stage):
    devices = range(lax.axis_size("chain"))
    return [
        lax.ppermute(value, "chain", [(i, i ^ (odd if i & 1 else even)) for i in devices])
        for odd, even in stage
    ]


def butterfly_sum(vector, width):
    for stage in stages(width):
        vector = sum(exchanged(vector, stage), vector)
    return vector


def kernel_and_sums(cost, final_marginal, marginals):
    rows, states = cost.shape
    tiles = states // LANES
    chunk = rows // CHUNKS

    def body(cost_ref, final_ref, marginal_ref, kernel_ref, sums_ref, scaled_ref, target_ref, sems, small_sems):
        def copy(index):
            span = pl.ds(index * chunk, chunk)
            return pltpu.make_async_copy(cost_ref.at[span], kernel_ref.at[span], sems.at[index])

        small = (
            pltpu.make_async_copy(final_ref, scaled_ref, small_sems.at[0]),
            pltpu.make_async_copy(marginal_ref, target_ref, small_sems.at[1]),
        )
        for index in range(CHUNKS):
            copy(index).start()
        for each in small:
            each.start()
        totals = [jnp.zeros((SUBLANES, LANES), jnp.float32)] * tiles
        for index in range(CHUNKS):
            copy(index).wait()
            if index == CHUNKS - 2:
                for each in small:
                    each.wait()
                final = scaled_ref[...]
                scaled_ref[...] = final * float(states)
                target_ref[...] = target_ref[...] * jnp.sum(final, keepdims=True)
            for first in range(index * chunk, (index + 1) * chunk, SUBLANES):
                for tile in range(tiles):
                    at = (pl.ds(first, SUBLANES), pl.ds(tile * LANES, LANES))
                    value = jnp.exp2(kernel_ref[at] * EXP2_SCALE)
                    kernel_ref[at] = value
                    totals[tile] = totals[tile] + value
        for tile in range(tiles):
            sums_ref[pl.ds(tile, 1), :] = jnp.sum(totals[tile], axis=0, keepdims=True)

    operands = (cost, final_marginal.reshape(tiles, LANES), marginals.reshape(rows // LANES, LANES))
    shapes = ((rows, states), (tiles, LANES), (tiles, LANES), (rows // LANES, LANES))
    return pl.pallas_call(
        body,
        out_shape=[jax.ShapeDtypeStruct(shape, jnp.float32) for shape in shapes],
        in_specs=[pl.BlockSpec(memory_space=pltpu.HBM)] * 3,
        out_specs=[pl.BlockSpec(memory_space=pltpu.VMEM)] * 4,
        scratch_shapes=[pltpu.SemaphoreType.DMA((CHUNKS,)), pltpu.SemaphoreType.DMA((2,))],
        compiler_params=pltpu.CompilerParams(vmem_limit_bytes=16 << 20),
        name="kernel_and_sums",
    )(*(pltpu.with_memory_space_constraint(operand, pltpu.HBM) for operand in operands))


def log_row_scaling(kernel, parts, scaled, target):
    rows, states = kernel.shape
    tiles = states // LANES

    def body(kernel_ref, scaled_ref, target_ref, *refs):
        *part_refs, out_ref, weight_ref = refs
        sums = sum((ref[...] for ref in part_refs[1:]), part_refs[0][...])
        weight_ref[...] = scaled_ref[...] / sums
        weights = [
            jnp.broadcast_to(weight_ref[pl.ds(tile, 1), :], (SUBLANES, LANES)) for tile in range(tiles)
        ]
        partial = []
        for first in range(0, rows, SUBLANES):
            sums = [None] * 4
            for tile in range(tiles):
                at = (pl.ds(first, SUBLANES), pl.ds(tile * LANES, LANES))
                term = kernel_ref[at] * weights[tile]
                sums[tile % 4] = term if sums[tile % 4] is None else sums[tile % 4] + term
            partial.append((sums[0] + sums[1]) + (sums[2] + sums[3]))
        for block in range(rows // LANES):
            square = jnp.concatenate(partial[block * 16 : block * 16 + 16], axis=0)
            row_sums = jnp.sum(square.T, axis=0, keepdims=True)
            at = (pl.ds(block, 1), slice(None))
            out_ref[at] = jnp.log(target_ref[at] / row_sums)

    return pl.pallas_call(
        body,
        out_shape=jax.ShapeDtypeStruct((rows // LANES, LANES), jnp.float32),
        in_specs=[pl.BlockSpec(memory_space=pltpu.VMEM)] * (3 + len(parts)),
        out_specs=pl.BlockSpec(memory_space=pltpu.VMEM),
        scratch_shapes=[pltpu.VMEM((tiles, LANES), jnp.float32)],
        compiler_params=pltpu.CompilerParams(vmem_limit_bytes=16 << 20),
        name="log_row_scaling",
    )(kernel, scaled, target, *parts).reshape(rows)


def summed_parts(sums, width):
    across = distances(width)
    if len(across) < 2:
        return [butterfly_sum(sums, width)]
    one, other, *rest = across
    both = one ^ other | 1
    for apart in rest:
        sums = sums + swapped(sums, "chain", apart)
    of_other_core = swapped(sums, "chain", 1)
    far = swapped(sums, "chain", both)
    whole = sums + of_other_core
    (near,) = exchanged(whole, [(one, other)])
    (side,) = exchanged(whole, [(other, one)])
    far_of_other_core = swapped(far, "chain", 1)
    return [whole, near, side, far, far_of_other_core]


def one_kernel(cost, marginals, final_marginal):
    width = cost.shape[1] // cost.shape[0]
    kernel, sums, scaled, target = kernel_and_sums(cost, final_marginal, marginals)
    return log_row_scaling(kernel, summed_parts(sums, width), scaled, target)


def from_behind(block, axis, distance):
    devices = range(lax.axis_size(axis))
    route = [(i - distance, i) for i in devices if i - distance in devices]
    return lax.ppermute(block, axis, route)


def doubling_gather(first, second, member, width):
    for bit_index in range(width.bit_length() - 1):
        other_first, other_second = (swapped(part, "chain", 1 << bit_index) for part in (first, second))
        upward = member >> bit_index & 1 == 1
        first = jnp.where(
            upward, jnp.concatenate([other_first, first]), jnp.concatenate([first, other_first])
        )
        second = jnp.where(
            upward, jnp.concatenate([other_second, second]), jnp.concatenate([second, other_second])
        )
    return (first, second)


def many_kernels(cost, marginals, final_marginal):
    row_count = cost.shape[0]
    states = cost.shape[1]
    width = states // row_count
    kernels = lax.axis_size("chain") // width
    index = lax.axis_index("chain")
    group = index // width
    member = index % width
    kernel = jnp.exp(-cost / entropic)
    scaling = jnp.ones((row_count,), jnp.float32)
    last_scaling = jnp.ones((states,), jnp.float32)
    for _ in range(SWEEPS):
        current = scaling
        alpha_start = jnp.ones((states,), jnp.float32)
        forward_state = (jnp.ones((row_count,), jnp.float32), current, alpha_start)
        backward_state = (jnp.ones((row_count,), jnp.float32), last_scaling)
        for position in range(kernels):
            partial_sums = jnp.dot(
                forward_state[1],
                kernel,
                precision=lax.Precision.HIGHEST,
                preferred_element_type=jnp.float32,
            )
            whole = butterfly_sum(partial_sums, width)
            forward_whole_alpha = whole * (states / jnp.sum(whole))
            forward_outgoing = lax.dynamic_slice_in_dim(
                forward_whole_alpha, member * row_count, row_count
            )
            forward_alpha_block, carried, forward_alpha_last = forward_state
            if position == kernels - 1:
                forward_alpha_last = forward_whole_alpha
            if position < kernels - 1:
                forward_arrived = from_behind(forward_outgoing, "chain", width)
                taking = group == position + 1
                forward_alpha_block = jnp.where(taking, forward_arrived, forward_alpha_block)
                carried = jnp.where(taking, current * forward_arrived, carried)
            forward_state = (forward_alpha_block, carried, forward_alpha_last)
        for position in range(kernels):
            backward_raw = jnp.dot(
                kernel,
                backward_state[1],
                precision=lax.Precision.HIGHEST,
                preferred_element_type=jnp.float32,
            )
            backward_raw_full, backward_weighted_full = doubling_gather(
                backward_raw, current * backward_raw, member, width
            )
            backward_beta_block, carried_full = backward_state
            target_step = kernels - 1 - position
            factor = states / jnp.sum(backward_raw_full)
            backward_beta_block = jnp.where(
                group == target_step, backward_raw * factor, backward_beta_block
            )
            if target_step > 0:
                arrived = from_behind(backward_weighted_full * factor, "chain", -width)
                carried_full = jnp.where(group == target_step - 1, arrived, carried_full)
            backward_state = (backward_beta_block, carried_full)
        alpha_block, _, alpha_last = forward_state
        beta_block = backward_state[0]
        scaling = marginals / (alpha_block * beta_block)
        last_scaling = final_marginal / alpha_last
    return jnp.log(scaling)


def on_device(cost, marginals, final_marginal):
    width = cost.shape[1] // cost.shape[0]
    if lax.axis_size("chain") == width:
        return one_kernel(cost, marginals, final_marginal)
    return many_kernels(cost, marginals, final_marginal)


def solution(mesh):
    placed = (P(("pop", "chain"), None), P(("pop", "chain")), P("pop"))
    return jax.shard_map(
        on_device, mesh=mesh, in_specs=placed, out_specs=P(("pop", "chain")), check_vma=False
    )
```

```python
import jax
import jax.numpy as jnp
from jax import lax
from jax.experimental import pallas as pl
from jax.experimental.pallas import tpu as pltpu
from jax.sharding import PartitionSpec as P

SWEEPS = 2
LANES = 128
SUBLANES = 8
PARTS = (8, 8, 8, 4, 2, 2)


entropic = 0.25
EXP2_SCALE = -1.4426950408889634 / entropic


def swapped(value, axis, apart):
    return lax.ppermute(value, axis, [(i, i ^ apart) for i in range(lax.axis_size(axis))])


def distances(width):
    return [1 << bit_index | 1 for bit_index in range(1, width.bit_length() - 1)]


def stages(width):
    across = distances(width)
    if len(across) < 2:
        return [[(apart, apart)] for apart in [*across, 1] if apart < width]
    one, other, *rest = across
    both = one ^ other | 1
    last = [(both, both), (one, other), (other, one)]
    return [*([(apart, apart)] for apart in rest), [(1, 1)], last]


def exchanged(value, stage):
    devices = range(lax.axis_size("chain"))
    return [
        lax.ppermute(value, "chain", [(i, i ^ (odd if i & 1 else even)) for i in devices])
        for odd, even in stage
    ]


def butterfly_sum(vector, width):
    for stage in stages(width):
        vector = sum(exchanged(vector, stage), vector)
    return vector


def kernel_and_sums(cost, final_marginal, marginals):
    rows, states = cost.shape
    tiles = states // LANES
    starts = [rows * sum(PARTS[:index]) // sum(PARTS) for index in range(len(PARTS) + 1)]

    def body(cost_ref, final_ref, marginal_ref, kernel_ref, sums_ref, scaled_ref, target_ref, sems, small_sems):
        def copy(index):
            span = pl.ds(starts[index], starts[index + 1] - starts[index])
            return pltpu.make_async_copy(cost_ref.at[span], kernel_ref.at[span], sems.at[index])

        small = (
            pltpu.make_async_copy(final_ref, scaled_ref, small_sems.at[0]),
            pltpu.make_async_copy(marginal_ref, target_ref, small_sems.at[1]),
        )
        for index in range(len(PARTS)):
            copy(index).start()
        for each in small:
            each.start()
        totals = [jnp.zeros((SUBLANES, LANES), jnp.float32)] * tiles
        for index in range(len(PARTS)):
            copy(index).wait()
            if index == len(PARTS) - 2:
                for each in small:
                    each.wait()
                final = scaled_ref[...]
                scaled_ref[...] = final * float(states)
                target_ref[...] = target_ref[...] * jnp.sum(final, keepdims=True)
            for first in range(starts[index], starts[index + 1], SUBLANES):
                for tile in range(tiles):
                    at = (pl.ds(first, SUBLANES), pl.ds(tile * LANES, LANES))
                    value = jnp.exp2(kernel_ref[at] * EXP2_SCALE)
                    kernel_ref[at] = value
                    totals[tile] = totals[tile] + value
        for tile in range(tiles):
            sums_ref[pl.ds(tile, 1), :] = jnp.sum(totals[tile], axis=0, keepdims=True)

    operands = (cost, final_marginal.reshape(tiles, LANES), marginals.reshape(rows // LANES, LANES))
    shapes = ((rows, states), (tiles, LANES), (tiles, LANES), (rows // LANES, LANES))
    return pl.pallas_call(
        body,
        out_shape=[jax.ShapeDtypeStruct(shape, jnp.float32) for shape in shapes],
        in_specs=[pl.BlockSpec(memory_space=pltpu.HBM)] * 3,
        out_specs=[pl.BlockSpec(memory_space=pltpu.VMEM)] * 4,
        scratch_shapes=[pltpu.SemaphoreType.DMA((len(PARTS),)), pltpu.SemaphoreType.DMA((2,))],
        compiler_params=pltpu.CompilerParams(vmem_limit_bytes=16 << 20),
        name="kernel_and_sums",
    )(*(pltpu.with_memory_space_constraint(operand, pltpu.HBM) for operand in operands))


def log_row_scaling(kernel, parts, scaled, target):
    rows, states = kernel.shape
    tiles = states // LANES

    def body(kernel_ref, scaled_ref, target_ref, *refs):
        *part_refs, out_ref, weight_ref = refs
        sums = sum((ref[...] for ref in part_refs[1:]), part_refs[0][...])
        weight_ref[...] = scaled_ref[...] / sums
        weights = [
            jnp.broadcast_to(weight_ref[pl.ds(tile, 1), :], (SUBLANES, LANES)) for tile in range(tiles)
        ]
        partial = []
        for first in range(0, rows, SUBLANES):
            sums = [None] * 4
            for tile in range(tiles):
                at = (pl.ds(first, SUBLANES), pl.ds(tile * LANES, LANES))
                term = kernel_ref[at] * weights[tile]
                sums[tile % 4] = term if sums[tile % 4] is None else sums[tile % 4] + term
            partial.append((sums[0] + sums[1]) + (sums[2] + sums[3]))
        for block in range(rows // LANES):
            square = jnp.concatenate(partial[block * 16 : block * 16 + 16], axis=0)
            row_sums = jnp.sum(square.T, axis=0, keepdims=True)
            at = (pl.ds(block, 1), slice(None))
            out_ref[at] = jnp.log(target_ref[at] / row_sums)

    return pl.pallas_call(
        body,
        out_shape=jax.ShapeDtypeStruct((rows // LANES, LANES), jnp.float32),
        in_specs=[pl.BlockSpec(memory_space=pltpu.VMEM)] * (3 + len(parts)),
        out_specs=pl.BlockSpec(memory_space=pltpu.VMEM),
        scratch_shapes=[pltpu.VMEM((tiles, LANES), jnp.float32)],
        compiler_params=pltpu.CompilerParams(vmem_limit_bytes=16 << 20),
        name="log_row_scaling",
    )(kernel, scaled, target, *parts).reshape(rows)


def summed_parts(sums, width):
    across = distances(width)
    if len(across) < 2:
        return [butterfly_sum(sums, width)]
    one, other, *rest = across
    both = one ^ other | 1
    for apart in rest:
        sums = sums + swapped(sums, "chain", apart)
    of_other_core = swapped(sums, "chain", 1)
    far = swapped(sums, "chain", both)
    whole = sums + of_other_core
    (near,) = exchanged(whole, [(one, other)])
    (side,) = exchanged(whole, [(other, one)])
    far_of_other_core = swapped(far, "chain", 1)
    return [whole, near, side, far, far_of_other_core]


def one_kernel(cost, marginals, final_marginal):
    width = cost.shape[1] // cost.shape[0]
    kernel, sums, scaled, target = kernel_and_sums(cost, final_marginal, marginals)
    return log_row_scaling(kernel, summed_parts(sums, width), scaled, target)


def from_behind(block, axis, distance):
    devices = range(lax.axis_size(axis))
    route = [(i - distance, i) for i in devices if i - distance in devices]
    return lax.ppermute(block, axis, route)


def doubling_gather(first, second, member, width):
    for bit_index in range(width.bit_length() - 1):
        other_first, other_second = (swapped(part, "chain", 1 << bit_index) for part in (first, second))
        upward = member >> bit_index & 1 == 1
        first = jnp.where(
            upward, jnp.concatenate([other_first, first]), jnp.concatenate([first, other_first])
        )
        second = jnp.where(
            upward, jnp.concatenate([other_second, second]), jnp.concatenate([second, other_second])
        )
    return (first, second)


def many_kernels(cost, marginals, final_marginal):
    row_count = cost.shape[0]
    states = cost.shape[1]
    width = states // row_count
    kernels = lax.axis_size("chain") // width
    index = lax.axis_index("chain")
    group = index // width
    member = index % width
    kernel = jnp.exp(-cost / entropic)
    scaling = jnp.ones((row_count,), jnp.float32)
    last_scaling = jnp.ones((states,), jnp.float32)
    for _ in range(SWEEPS):
        current = scaling
        alpha_start = jnp.ones((states,), jnp.float32)
        forward_state = (jnp.ones((row_count,), jnp.float32), current, alpha_start)
        backward_state = (jnp.ones((row_count,), jnp.float32), last_scaling)
        for position in range(kernels):
            partial_sums = jnp.dot(
                forward_state[1],
                kernel,
                precision=lax.Precision.HIGHEST,
                preferred_element_type=jnp.float32,
            )
            whole = butterfly_sum(partial_sums, width)
            forward_whole_alpha = whole * (states / jnp.sum(whole))
            forward_outgoing = lax.dynamic_slice_in_dim(
                forward_whole_alpha, member * row_count, row_count
            )
            forward_alpha_block, carried, forward_alpha_last = forward_state
            if position == kernels - 1:
                forward_alpha_last = forward_whole_alpha
            if position < kernels - 1:
                forward_arrived = from_behind(forward_outgoing, "chain", width)
                taking = group == position + 1
                forward_alpha_block = jnp.where(taking, forward_arrived, forward_alpha_block)
                carried = jnp.where(taking, current * forward_arrived, carried)
            forward_state = (forward_alpha_block, carried, forward_alpha_last)
        for position in range(kernels):
            backward_raw = jnp.dot(
                kernel,
                backward_state[1],
                precision=lax.Precision.HIGHEST,
                preferred_element_type=jnp.float32,
            )
            backward_raw_full, backward_weighted_full = doubling_gather(
                backward_raw, current * backward_raw, member, width
            )
            backward_beta_block, carried_full = backward_state
            target_step = kernels - 1 - position
            factor = states / jnp.sum(backward_raw_full)
            backward_beta_block = jnp.where(
                group == target_step, backward_raw * factor, backward_beta_block
            )
            if target_step > 0:
                arrived = from_behind(backward_weighted_full * factor, "chain", -width)
                carried_full = jnp.where(group == target_step - 1, arrived, carried_full)
            backward_state = (backward_beta_block, carried_full)
        alpha_block, _, alpha_last = forward_state
        beta_block = backward_state[0]
        scaling = marginals / (alpha_block * beta_block)
        last_scaling = final_marginal / alpha_last
    return jnp.log(scaling)


def on_device(cost, marginals, final_marginal):
    width = cost.shape[1] // cost.shape[0]
    if lax.axis_size("chain") == width:
        return one_kernel(cost, marginals, final_marginal)
    return many_kernels(cost, marginals, final_marginal)


def solution(mesh):
    placed = (P(("pop", "chain"), None), P(("pop", "chain")), P("pop"))
    return jax.shard_map(
        on_device, mesh=mesh, in_specs=placed, out_specs=P(("pop", "chain")), check_vma=False
    )
```
